128 devices in a mesh: blk: 16 (over y_hi, x, core), red: 8 (over y_lo, z).
Axes of the slice: x: 4, y: 4 (y_hi: 2, y_lo: 2; y = y_hi * 2 + y_lo), z: 4, core: 2. Of those that a mesh axis runs over, the one named last changes fastest.
Arguments:
- x_now: bfloat16 [1024, 131072], P('blk', 'red'), may hold values from -6 to 6
- x_prev: float32 [1024, 131072], P('blk', 'red'), may hold values from -6 to 6
- density: float32 [1024, 131072], P('blk', 'red'), may hold values from -6 to 6
- coeffs: float32 [8], replicated, may hold values from -1 to 1
- potential: int32 [64], P('blk'), may hold values from 0 to 7
- h_tiles: bfloat16 [16, 96, 256, 256], P('blk', 'red'), may hold values from -0.1796875 to 0.1796875
- tile_rows: int32 [16, 96], P('blk', 'red'), may hold values from 0 to 31
- tile_cols: int32 [16, 96], P('blk', 'red'), may hold values from 0 to 63, as said below
- tile_counts: int32 [16, 8], P('blk', 'red'), may hold values from 3 to 12, as said below
Outputs:
- x_next: float32 [1024, 131072], P('blk', 'red')
- density_out: float32 [1024, 131072], P('blk', 'red')
The draws below stay inside these ranges and needn't reach their ends.
Inputs may be any that keep to these rules, and one draw needn't show every extreme that they name: `tile_cols`: block column within the group; the live slots of one panel and group name distinct positions (row, column). `tile_counts`: at most 12 live slots; some panel and group is full in every draw.
All inputs are finite; a program needn't handle non-finite values.
Results may differ from the reference program's by a relative error of at most 0.005.
Values may be sent and summed in bfloat16 or wider, within the bound.
A program may use at most 128 MiB of HBM per device.

```python
import jax
import jax.numpy as jnp
from jax import lax

BS = 256
ORDER = 131072
NMU = 8
SLAB_W = 16
CAP = 12
NB = 512
RB = 32
CB = 64
SLABS = 64
COLS = 1024
N_BLK = 16
N_RED = 8


def tile_layout(key):
    slices = N_BLK * N_RED
    places = RB * CB
    scores = jax.random.randint(jax.random.fold_in(key, 11), (slices, places), 0, 100000) * places + jnp.arange(places, dtype=jnp.int32)[None, :]
    unused, picks = lax.top_k(scores, CAP)
    picks = picks.astype(jnp.int32)
    row_ids = (picks // CB).reshape(N_BLK, N_RED * CAP)
    col_ids = (picks % CB).reshape(N_BLK, N_RED * CAP)
    return (row_ids, col_ids)


def draw_tile_rows(key, part):
    return tile_layout(key)[0]


def draw_tile_cols(key, part):
    return tile_layout(key)[1]


def draw_tile_counts(key, part):
    slices = N_BLK * N_RED
    counts = jax.random.randint(jax.random.fold_in(key, 23), (slices,), max(1, CAP // 4), CAP + 1)
    forced = jax.random.randint(jax.random.fold_in(key, 29), (), 0, slices)
    counts = jnp.where(jnp.arange(slices, dtype=jnp.int32) == forced, CAP, counts)
    return counts.astype(jnp.int32).reshape(N_BLK, N_RED)


def plant(values, rng, smallest, top_value):
    extent = values.shape
    spot = [jax.random.randint(jax.random.fold_in(rng, axis), (), 0, extent[axis]) for axis in range(len(extent))]
    values = values.at[tuple(spot)].set(smallest)
    longest = extent.index(max(extent))
    spot[longest] = (spot[longest] + 1) % extent[longest]
    return values.at[tuple(spot)].set(top_value)


def levels(rng, dims, split, smallest, top_value):
    gain, own = 1.0, jax.random.fold_in(rng, 6)
    for dim, blocks in split:
        steps = jnp.exp(jax.random.uniform(jax.random.fold_in(own, dim), (blocks,), jnp.float32, smallest / len(split), top_value / len(split)))
        gain = gain * jnp.repeat(steps, dims[dim] // blocks).reshape([-1 if axis == dim else 1 for axis in range(len(dims))])
    return gain


def noise(own_key, dims, scale, reach, pieces=(), kind=jnp.bfloat16):
    factor_of = levels(own_key, dims, pieces, -0.22, 0.18) if pieces else 1.0
    entries = jax.random.normal(own_key, dims, jnp.float32) * scale * factor_of
    return jnp.minimum(jnp.maximum(entries, -reach), reach).astype(kind)


def setup_inputs(seed: int = 0) -> dict:
    key_list = jax.random.split(jax.random.key(seed), 10)
    x_now = noise(key_list[0], (COLS, ORDER), 1.0, 6.0, ((0, 16), (1, 8)))
    x_prev = noise(key_list[1], (COLS, ORDER), 1.0, 6.0, ((0, 16), (1, 8)), jnp.float32)
    density = noise(key_list[2], (COLS, ORDER), 1.0, 6.0, ((0, 16), (1, 8)), jnp.float32)
    coeffs = jnp.clip(jax.random.uniform(key_list[3], (NMU,), jnp.float32, -1.0, 1.0), -1.0, 1.0)
    potential = plant(jax.random.randint(key_list[4], (SLABS,), 0, NMU), jax.random.fold_in(key_list[4], 1), 0, NMU - 1).astype(jnp.int32)
    h_tiles = noise(key_list[5], (N_BLK, N_RED * CAP, BS, BS), 0.03, 0.1796875, ((0, 16), (1, 8)))
    tile_rows = draw_tile_rows(jax.random.fold_in(key_list[9], 71), 0)
    tile_cols = draw_tile_cols(jax.random.fold_in(key_list[9], 71), 0)
    tile_counts = draw_tile_counts(jax.random.fold_in(key_list[9], 71), 0)
    return {"x_now": x_now, "x_prev": x_prev, "density": density, "coeffs": coeffs, "potential": potential, "h_tiles": h_tiles, "tile_rows": tile_rows, "tile_cols": tile_cols, "tile_counts": tile_counts}


def group_partial(x_blocks, tile_data, row_ids, col_ids, live_count, group):
    def one_panel(inputs):
        panel_tiles, panel_rows, panel_cols, panel_count = inputs
        picked = jnp.take(x_blocks, group * CB + panel_cols, axis=1).astype(jnp.float32)
        product = jnp.einsum("vck,cik->cvi", picked, panel_tiles.astype(jnp.float32))
        is_live = jnp.arange(CAP, dtype=jnp.int32) < panel_count
        placing = ((panel_rows[:, None] == jnp.arange(RB, dtype=jnp.int32)[None, :]) & is_live[:, None]).astype(jnp.float32)
        return jnp.einsum("cr,cvi->vri", placing, product, precision=lax.Precision.HIGHEST)

    stacked = lax.map(one_panel, (tile_data, row_ids, col_ids, live_count))
    return jnp.transpose(stacked, (1, 0, 2, 3)).reshape(COLS, ORDER)


def reference(x_now, x_prev, density, coeffs, potential, h_tiles, tile_rows, tile_cols, tile_counts):
    x_blocks = x_now.reshape(COLS, NB, BS)
    product = jnp.zeros((COLS, ORDER), jnp.float32)
    for group in range(N_RED):
        lower = group * CAP
        upper = lower + CAP
        partial_value = group_partial(x_blocks, h_tiles[:, lower:upper], tile_rows[:, lower:upper], tile_cols[:, lower:upper], tile_counts[:, group], group)
        rounded = lax.optimization_barrier(partial_value.astype(jnp.bfloat16))
        product = product + rounded.astype(jnp.float32)
    x_next = 2.0 * product - x_prev
    picking = (potential[:, None] == jnp.arange(NMU, dtype=jnp.int32)[None, :]).astype(jnp.float32)
    slab_coef = jnp.sum(picking * coeffs[None, :], axis=1)
    column_coef = jnp.repeat(slab_coef, SLAB_W)
    density_out = density + column_coef[:, None] * x_next
    return x_next, density_out
```

```python
import functools

import jax
import jax.numpy as jnp
from jax import lax
from jax.experimental import pallas as pl
from jax.experimental.pallas import tpu as pltpu
from jax.sharding import PartitionSpec as P

MESH = pl.DeviceIdType.MESH
NX = 4
LAG = 3
CHUNK = 3


def place():
    blk = lax.axis_index("blk")
    red = lax.axis_index("red")
    core = lax.rem(blk, 2)
    x = lax.rem(blk // 2, NX)
    yh = blk // (2 * NX)
    yl = red // NX
    z = lax.rem(red, NX)
    return x, yh, yl, z, core


def device(x, y, z, core):
    return ((y // 2) * (2 * NX) + x * 2 + core, lax.rem(y, 2) * NX + z)


def wrap(value):
    return lax.rem(value + 2 * NX, NX)


def exchange(cap, slab, bs, x_ref, h_ref, m_ref, out_ref, mout_ref, near_x, far_x, hb, cb, mbuf, msm,
             xs_sem, xr_sem, xl_sem, ys_sem, yr_sem, rs_sem, rr_sem, fs_sem, cs_sem, cr_sem,
             ms_sem, mr_sem, ns_sem, nr_sem, sm_sem):
    x, yh, yl, z, core = place()
    y = yh * 2 + yl
    other = 1 - core
    total = 2 * cap
    outer = jnp.logical_or(y == 0, y == 3)
    inner = jnp.logical_not(outer)

    def remote(src, dst, send, recv, to):
        return pltpu.make_async_remote_copy(
            src_ref=src, dst_ref=dst, send_sem=send, recv_sem=recv, device_id=to, device_id_type=MESH
        )

    here = (lax.axis_index("blk"), lax.axis_index("red"))
    sibling = device(x, y, z, other)
    x_up = device(wrap(x + 1), y, z, core)
    x_down = device(wrap(x - 1), y, z, core)
    y_pair = yh * 2 + (1 - yl)
    pair = device(x, y_pair, z, core)

    barrier = pltpu.get_barrier_semaphore()
    greeted = 0
    for dx in range(NX):
        for dy in range(NX):
            if dx or dy:
                pl.semaphore_signal(barrier, inc=1, device_id=device(wrap(x + dx), wrap(y + dy), z, core),
                                    device_id_type=MESH)
                greeted += 1
    for dz in range(NX):
        for dc in range(2):
            if dz or dc:
                to = device(x, y, wrap(z + dz), other if dc else core)
                pl.semaphore_signal(barrier, inc=1, device_id=to, device_id_type=MESH)
                greeted += 1
    blocks = near_x.shape[1]

    def load_x(b, carry):
        columns = pl.ds(pl.multiple_of(b * bs, bs), bs)
        pltpu.make_async_copy(x_ref.at[:, columns], near_x.at[core, b], xl_sem).start()
        return carry

    lax.fori_loop(0, blocks, load_x, 0)
    own_x = pltpu.make_async_copy(far_x.at[core], near_x.at[core], xl_sem)

    @pl.when(outer)
    def _():
        def load(t, carry):
            pltpu.make_async_copy(h_ref.at[0, t], hb.at[0, 0, t], yr_sem.at[0, t]).start()
            return carry
        lax.fori_loop(0, cap, load, 0)

    pl.semaphore_wait(barrier, greeted)

    group = jnp.where(outer, 0, 1)
    for d in range(NX):
        for half in range(2):
            y_to = half * 2 + yh
            to = device(wrap(x - d), y_to, z, core)
            if d == 0:
                @pl.when(y_to != y)
                def _(to=to, d=d, half=half):
                    remote(m_ref, mbuf.at[group, d], ms_sem.at[half, d], mr_sem.at[group, d], to).start()

                @pl.when(y_to == y)
                def _(d=d):
                    pltpu.make_async_copy(m_ref, mbuf.at[group, d], mr_sem.at[group, d]).start()
            else:
                remote(m_ref, mbuf.at[group, d], ms_sem.at[half, d], mr_sem.at[group, d], to).start()

    own_x.wait()
    to_sibling = remote(near_x.at[core], near_x.at[core], xs_sem.at[0], xr_sem.at[0], sibling)
    to_sibling.start()
    to_pair = remote(near_x.at[core], far_x.at[core], xs_sem.at[1], xr_sem.at[1], pair)
    forward_x = remote(far_x.at[core], far_x.at[core], xs_sem.at[2], xr_sem.at[2], sibling)
    far = device(x, wrap(y + 2), z, core)
    near = (device(x, y_pair, z, core), device(x, wrap(y_pair + 2), z, core))

    @pl.when(outer)
    def _():
        def send(t, carry):
            remote(h_ref.at[0, t], hb.at[0, 0, t], ys_sem.at[0], yr_sem.at[0, t], far).start()
            return carry
        lax.fori_loop(0, cap, send, 0)
        to_pair.start()

    @pl.when(inner)
    def _():
        to_pair.start()

        def send(t, carry):
            for n in range(2):
                remote(h_ref.at[0, t], hb.at[1, 0, t], ys_sem.at[n], yr_sem.at[1, t], near[n]).start()
            return carry
        lax.fori_loop(0, cap, send, 0)

    for s in range(2):
        for d in range(NX):
            pltpu.make_async_copy(m_ref, mbuf.at[s, d], mr_sem.at[s, d]).wait()
    into_smem = pltpu.make_async_copy(mbuf, msm, sm_sem)
    into_smem.start()
    to_sibling.wait_recv()
    into_smem.wait()

    def side(s):
        return jnp.where(s == 0, yl, 1 - yl)

    for s in range(2):
        for dz in range(NX):
            z_to = wrap(z + dz)
            d = wrap(z_to - x)
            for dc in range(2):
                if dz or dc:
                    to = device(x, y, z_to, other if dc else core)
                    remote(mbuf.at[s, d], mout_ref.at[core, side(s), z], ns_sem.at[s, dz, dc],
                           nr_sem.at[core, side(s), z], to).start()
                else:
                    pltpu.make_async_copy(mbuf.at[s, d], mout_ref.at[core, side(s), z],
                                          nr_sem.at[core, side(s), z]).start()

    def send_chunk(q):
        s = q // (cap // CHUNK)
        first = lax.rem(q, cap // CHUNK) * CHUNK
        slots = pl.ds(first, CHUNK)
        for dz in range(NX):
            z_to = wrap(z + dz)
            d = wrap(z_to - x)
            for dc in range(2):
                c_to = other if dc else core
                src = cb.at[s, d, c_to, slots]
                dst = out_ref.at[core, side(s), z, slots]
                arrived = cr_sem.at[core, side(s), z]
                if dz or dc:
                    remote(src, dst, cs_sem.at[s, dz, dc], arrived, device(x, y, z_to, c_to)).start()
                else:
                    pltpu.make_async_copy(src, dst, arrived).start()

    def multiply(s, t, carry):
        k = s * cap + t
        held_x = far_x if s else near_x

        @pl.when(jnp.logical_and(lax.rem(k, CHUNK) == 0, k > 0))
        def _():
            send_chunk(k // CHUNK - 1)

        if s:
            @pl.when(t == 0)
            def _():
                to_pair.wait_recv()
                forward_x.start()
                forward_x.wait_recv()

        pltpu.make_async_copy(h_ref.at[0, 0], hb.at[s, 2, t], rr_sem.at[2, k]).wait()
        for d in range(NX):
            column = msm[s, d, 0, t]
            picked = jnp.concatenate([held_x[0, column], held_x[1, column]], axis=0)
            product = lax.dot_general(
                picked, hb[s, d, t], (((1,), (1,)), ((), ())), preferred_element_type=jnp.float32
            ).astype(jnp.bfloat16)
            cb[s, d, 0, t] = product[:slab]
            cb[s, d, 1, t] = product[slab:]
        return carry

    def reach(i):
        free = i - 2 * LAG + 1
        held = jnp.where(jnp.logical_and(inner, i < cap + 2 * LAG + 3), jnp.minimum(free, cap), free)
        return jnp.clip(held, 0, total)

    def step(i, carry):
        @pl.when(i < total)
        def _():
            s = i // cap
            t = lax.rem(i, cap)
            pltpu.make_async_copy(h_ref.at[0, 0], hb.at[s, 0, t], yr_sem.at[s, t]).wait()
            mine = hb.at[s, 0, t]
            remote(mine, hb.at[s, 3, t], rs_sem.at[0, s], rr_sem.at[3, i], x_up).start()
            remote(mine, hb.at[s, 1, t], rs_sem.at[1, s], rr_sem.at[1, i], x_down).start()

        @pl.when(jnp.logical_and(i >= LAG, i < total + LAG))
        def _():
            j = i - LAG
            s = j // cap
            t = lax.rem(j, cap)
            for d in (1, 3):
                pltpu.make_async_copy(h_ref.at[0, 0], hb.at[s, d, t], rr_sem.at[d, j]).wait()

            @pl.when(lax.rem(j, 2) == 0)
            def _():
                remote(hb.at[s, 3, t], hb.at[s, 2, t], fs_sem.at[0, s], rr_sem.at[2, j], x_up).start()

            @pl.when(lax.rem(j, 2) == 1)
            def _():
                remote(hb.at[s, 1, t], hb.at[s, 2, t], fs_sem.at[1, s], rr_sem.at[2, j], x_down).start()

        done, until = reach(i - 1), reach(i)
        lax.fori_loop(jnp.minimum(done, cap), jnp.minimum(until, cap), functools.partial(multiply, 0), 0)
        lax.fori_loop(jnp.maximum(done - cap, 0), jnp.maximum(until - cap, 0), functools.partial(multiply, 1), 0)
        return carry

    lax.fori_loop(0, total + 2 * LAG, step, 0)

    to_sibling.wait_send()
    to_pair.wait_send()
    forward_x.wait_send()
    pltpu.make_async_copy(h_ref.at[0], hb.at[0, 0], ys_sem.at[0]).wait()

    @pl.when(inner)
    def _():
        pltpu.make_async_copy(h_ref.at[0], hb.at[0, 0], ys_sem.at[1]).wait()

    send_chunk(jnp.int32(total // CHUNK - 1))
    for way in range(2):
        for s in range(2):
            pltpu.make_async_copy(h_ref.at[0], hb.at[s, 0], rs_sem.at[way, s]).wait()
            pltpu.make_async_copy(h_ref.at[0, pl.ds(0, cap // 2)], hb.at[s, 0, pl.ds(0, cap // 2)],
                                  fs_sem.at[way, s]).wait()
    for half in range(2):
        for d in range(NX):
            if d == 0:
                @pl.when(half * 2 + yh != y)
                def _(half=half, d=d):
                    pltpu.make_async_copy(m_ref, mbuf.at[0, 0], ms_sem.at[half, d]).wait()
            else:
                pltpu.make_async_copy(m_ref, mbuf.at[0, 0], ms_sem.at[half, d]).wait()
    for s in range(2):
        for dz in range(NX):
            for dc in range(2):
                if dz or dc:
                    pltpu.make_async_copy(mbuf.at[0, 0], mout_ref.at[0, 0, 0], ns_sem.at[s, dz, dc]).wait()
                    pltpu.make_async_copy(cb.at[0, 0, 0], out_ref.at[0, 0, 0], cs_sem.at[s, dz, dc]).wait()
    for c in range(2):
        for g in range(2):
            for q in range(NX):
                pltpu.make_async_copy(mbuf.at[0, 0], mout_ref.at[c, g, q], nr_sem.at[c, g, q]).wait()
                pltpu.make_async_copy(cb.at[0, 0, 0], out_ref.at[c, g, q], cr_sem.at[c, g, q]).wait()


def combine(cap, bs, slabs, steps, meta, coeffs, potential, c_ref, prev_ref, dens_ref, next_ref, dout_ref, acc):
    panel = pl.program_id(0)
    part = pl.program_id(1)
    columns = prev_ref.shape[0]
    width = prev_ref.shape[1]

    @pl.when(part == 0)
    def _():
        acc[...] = jnp.zeros_like(acc)
        for g in range(2):
            for q in range(NX):
                for t in range(cap):
                    row = pl.multiple_of(meta[panel, g, q, 1, t] * bs, bs)
                    acc[:, pl.ds(row, bs)] += c_ref[0, g, q, t].astype(jnp.float32)

    height = columns // slabs
    base = pl.multiple_of(part * width, width)
    for s in range(slabs):
        rows = pl.ds(s * height, height)
        value = 2.0 * acc[rows, pl.ds(base, width)] - prev_ref[rows, :]
        next_ref[rows, :] = value
        dout_ref[rows, :] = dens_ref[rows, :] + coeffs[potential[s]] * value


def shards(x_now, x_prev, density, coeffs, potential, h_tiles, tile_rows, tile_cols, tile_counts):
    columns, local_rows = x_now.shape
    cap = h_tiles.shape[1]
    bs = h_tiles.shape[-1]
    slabs = potential.shape[0]
    panel_rows = local_rows // bs // 2
    live = jnp.arange(cap, dtype=jnp.int32)[None, :] < tile_counts
    rows = jnp.where(live, tile_rows, panel_rows)
    lane_pad = ((0, 0), (0, 128 - cap))
    meta = jnp.concatenate([jnp.pad(tile_cols, lane_pad), jnp.pad(rows, lane_pad),
                            jnp.zeros((6, 128), jnp.int32)], axis=0)
    dma = pltpu.SemaphoreType.DMA
    bf16 = jnp.bfloat16
    anywhere = pl.BlockSpec(memory_space=pl.ANY)
    flops = 2 * 8 * cap * 2 * columns * bs * bs
    sums, places = pl.pallas_call(
        functools.partial(exchange, cap, columns, bs),
        out_shape=(
            jax.ShapeDtypeStruct((2, 2, NX, cap, columns, bs), bf16),
            jax.ShapeDtypeStruct((2, 2, NX, 8, 128), jnp.int32),
        ),
        in_specs=[anywhere, anywhere, pl.BlockSpec(memory_space=pltpu.VMEM)],
        out_specs=(anywhere, anywhere),
        scratch_shapes=[
            pltpu.VMEM((2, local_rows // bs, columns, bs), bf16),
            pltpu.VMEM((2, local_rows // bs, columns, bs), bf16),
            pltpu.VMEM((2, NX, cap, bs, bs), bf16),
            pltpu.VMEM((2, NX, 2, cap, columns, bs), bf16),
            pltpu.VMEM((2, NX, 8, 128), jnp.int32),
            pltpu.SMEM((2, NX, 8, 128), jnp.int32),
            dma((3,)), dma((3,)), dma,
            dma((2,)), dma((2, cap)),
            dma((2, 2)), dma((4, 2 * cap)), dma((2, 2)),
            dma((2, NX, 2)), dma((2, 2, NX)),
            dma((2, NX)), dma((2, NX)),
            dma((2, NX, 2)), dma((2, 2, NX)), dma,
        ],
        compiler_params=pltpu.CompilerParams(
            collective_id=0, has_side_effects=True, vmem_limit_bytes=56 * 1024 * 1024
        ),
        cost_estimate=pl.CostEstimate(flops=flops, bytes_accessed=16 * 1024 * 1024, transcendentals=0),
        name="exchange",
    )(x_now, h_tiles, meta)
    parts = 4
    width = local_rows // 2 // parts
    wide = pl.BlockSpec((columns, width), lambda p, i, *_: (0, p * parts + i))
    return tuple(pl.pallas_call(
        functools.partial(combine, cap, bs, slabs, parts),
        out_shape=(
            jax.ShapeDtypeStruct((columns, local_rows), jnp.float32),
            jax.ShapeDtypeStruct((columns, local_rows), jnp.float32),
        ),
        grid_spec=pltpu.PrefetchScalarGridSpec(
            num_scalar_prefetch=3,
            grid=(2, parts),
            in_specs=[
                pl.BlockSpec((1, 2, NX, cap, columns, bs), lambda p, i, *_: (p, 0, 0, 0, 0, 0)),
                wide, wide,
            ],
            out_specs=(wide, wide),
            scratch_shapes=[pltpu.VMEM((columns, (panel_rows + 1) * bs), jnp.float32)],
        ),
        compiler_params=pltpu.CompilerParams(vmem_limit_bytes=48 * 1024 * 1024),
        cost_estimate=pl.CostEstimate(flops=8 * columns * local_rows, bytes_accessed=24 * 1024 * 1024,
                                      transcendentals=0),
        name="combine",
    )(places, coeffs, potential, sums, x_prev, density))


def solution(mesh):
    in_specs = (
        P("blk", "red"),
        P("blk", "red"),
        P("blk", "red"),
        P(),
        P("blk"),
        P("blk", "red", None, None),
        P("blk", "red"),
        P("blk", "red"),
        P("blk", "red"),
    )
    out_specs = (P("blk", "red"), P("blk", "red"))
    return jax.shard_map(shards, mesh=mesh, in_specs=in_specs, out_specs=out_specs, check_vma=False)
```

```python
import functools

import jax
import jax.numpy as jnp
from jax import lax
from jax.experimental import pallas as pl
from jax.experimental.pallas import tpu as pltpu
from jax.sharding import PartitionSpec as P

MESH = pl.DeviceIdType.MESH
NX = 4
LAG = 4
CHUNK = 1
HOLD = 12


def place():
    blk = lax.axis_index("blk")
    red = lax.axis_index("red")
    core = lax.rem(blk, 2)
    x = lax.rem(blk // 2, NX)
    yh = blk // (2 * NX)
    yl = red // NX
    z = lax.rem(red, NX)
    return x, yh, yl, z, core


def device(x, y, z, core):
    return ((y // 2) * (2 * NX) + x * 2 + core, lax.rem(y, 2) * NX + z)


def wrap(value):
    return lax.rem(value + 2 * NX, NX)


def exchange(cap, slab, bs, x_ref, h_ref, cols_ref, rows_ref, count_ref, out_ref, mout_ref, first_x, second_x, hb, cb, m_own, mbuf, msm,
             xs_sem, xr_sem, xl_sem, ys_sem, yr_sem, rs_sem, rr_sem, fs_sem, cs_sem, cr_sem,
             ms_sem, mr_sem, ns_sem, nr_sem, sm_sem):
    x, yh, yl, z, core = place()
    y = yh * 2 + yl
    other = 1 - core
    total = 2 * cap
    outer = jnp.logical_or(y == 0, y == 3)
    inner = jnp.logical_not(outer)

    def remote(src, dst, send, recv, to):
        return pltpu.make_async_remote_copy(
            src_ref=src, dst_ref=dst, send_sem=send, recv_sem=recv, device_id=to, device_id_type=MESH
        )

    here = (lax.axis_index("blk"), lax.axis_index("red"))
    sibling = device(x, y, z, other)
    x_up = device(wrap(x + 1), y, z, core)
    x_down = device(wrap(x - 1), y, z, core)
    y_pair = yh * 2 + (1 - yl)
    pair = device(x, y_pair, z, core)

    barrier = pltpu.get_barrier_semaphore()
    greeted = 0
    for dx in range(NX):
        for dy in range(NX):
            if dx or dy:
                pl.semaphore_signal(barrier, inc=1, device_id=device(wrap(x + dx), wrap(y + dy), z, core),
                                    device_id_type=MESH)
                greeted += 1
    for dz in range(NX):
        for dc in range(2):
            if dz or dc:
                to = device(x, y, wrap(z + dz), other if dc else core)
                pl.semaphore_signal(barrier, inc=1, device_id=to, device_id_type=MESH)
                greeted += 1
    blocks = first_x.shape[1]
    m_ref = m_own
    m_ref[...] = jnp.zeros(m_ref.shape, m_ref.dtype)
    m_ref[0:1, 0:cap] = cols_ref[...]
    m_ref[1:2, 0:cap] = rows_ref[...]
    m_ref[2:3, 0:1] = count_ref[...]

    def load_x(held):
        def one(b, carry):
            columns = pl.ds(pl.multiple_of(b * bs, bs), bs)
            pltpu.make_async_copy(x_ref.at[:, columns], held.at[core, b], xl_sem).start()
            return carry
        lax.fori_loop(0, blocks, one, 0)

    @pl.when(outer)
    def _():
        load_x(first_x)

    @pl.when(inner)
    def _():
        load_x(second_x)

    own_x = pltpu.make_async_copy(second_x.at[core], first_x.at[core], xl_sem)

    @pl.when(outer)
    def _():
        def load(t, carry):
            pltpu.make_async_copy(h_ref.at[0, t], hb.at[0, 0, t], yr_sem.at[0, t]).start()
            return carry
        lax.fori_loop(0, cap, load, 0)

    pl.semaphore_wait(barrier, greeted)

    for d in range(NX):
        for half in range(2):
            y_to = half * 2 + yh
            to_outer = jnp.logical_or(y_to == 0, y_to == 3)
            phase = jnp.where(to_outer == outer, 0, 1)
            to = device(wrap(x - d), y_to, z, core)
            if d == 0:
                @pl.when(y_to != y)
                def _(to=to, d=d, half=half, phase=phase):
                    remote(m_ref, mbuf.at[phase, d], ms_sem.at[half, d], mr_sem.at[phase, d], to).start()

                @pl.when(y_to == y)
                def _(d=d, phase=phase):
                    pltpu.make_async_copy(m_ref, mbuf.at[phase, d], mr_sem.at[phase, d]).start()
            else:
                remote(m_ref, mbuf.at[phase, d], ms_sem.at[half, d], mr_sem.at[phase, d], to).start()

    own_x.wait()
    far = device(x, wrap(y + 2), z, core)
    near = (pair, device(x, wrap(y_pair + 2), z, core))

    def x_copies(own, other_x):
        return (
            remote(own.at[core], own.at[core], xs_sem.at[0], xr_sem.at[0], sibling),
            remote(own.at[core], own.at[core], xs_sem.at[1], xr_sem.at[1], pair),
            remote(other_x.at[core], other_x.at[core], xs_sem.at[2], xr_sem.at[2], sibling),
        )

    to_sibling, to_pair, forward_x = x_copies(first_x, second_x)
    to_sibling_in, to_pair_in, forward_x_in = x_copies(second_x, first_x)

    @pl.when(outer)
    def _():
        to_pair.start()
        to_sibling.start()

        def send(t, carry):
            remote(h_ref.at[0, t], hb.at[1, 0, t], ys_sem.at[0], yr_sem.at[1, t], far).start()
            return carry
        lax.fori_loop(0, cap, send, 0)

    @pl.when(inner)
    def _():
        to_pair_in.start()
        to_sibling_in.start()

        def send(t, carry):
            remote(h_ref.at[0, t], hb.at[0, 0, t], ys_sem.at[1], yr_sem.at[0, t], near[1]).start()
            return carry
        lax.fori_loop(0, cap, send, 0)

        def send_near(t, carry):
            remote(h_ref.at[0, t], hb.at[1, 0, t], ys_sem.at[0], yr_sem.at[1, t], near[0]).start()
            return carry
        lax.fori_loop(0, cap, send_near, 0)

    for s in range(2):
        for d in range(NX):
            pltpu.make_async_copy(m_ref, mbuf.at[s, d], mr_sem.at[s, d]).wait()
    into_smem = pltpu.make_async_copy(mbuf, msm, sm_sem)
    into_smem.start()
    to_sibling.wait_recv()
    into_smem.wait()

    def side(s):
        return jnp.where((s == 0) == outer, yl, 1 - yl)

    for s in range(2):
        for dz in range(NX):
            z_to = wrap(z + dz)
            d = wrap(z_to - x)
            for dc in range(2):
                if dz or dc:
                    to = device(x, y, z_to, other if dc else core)
                    remote(mbuf.at[s, d], mout_ref.at[core, side(s), z], ns_sem.at[s, dz, dc],
                           nr_sem.at[core, side(s), z], to).start()
                else:
                    pltpu.make_async_copy(mbuf.at[s, d], mout_ref.at[core, side(s), z],
                                          nr_sem.at[core, side(s), z]).start()

    def send_chunk(q):
        s = q // (cap // CHUNK)
        first = lax.rem(q, cap // CHUNK) * CHUNK
        slots = pl.ds(first, CHUNK)
        for dz in range(NX):
            z_to = wrap(z + dz)
            d = wrap(z_to - x)
            for dc in range(2):
                c_to = other if dc else core
                src = cb.at[s, d, c_to, slots]
                dst = out_ref.at[core, side(s), z, slots]
                arrived = cr_sem.at[core, side(s), z]
                if dz or dc:
                    remote(src, dst, cs_sem.at[s, dz, dc], arrived, device(x, y, z_to, c_to)).start()
                else:
                    pltpu.make_async_copy(src, dst, arrived).start()

    def multiply(s, t, carry):
        k = s * cap + t
        held_x = second_x if s else first_x

        @pl.when(jnp.logical_and(lax.rem(k, CHUNK) == 0, k > 0))
        def _():
            send_chunk(k // CHUNK - 1)

        crossed = forward_x if s else forward_x_in

        @pl.when(jnp.logical_and(t == 0, outer if s else inner))
        def _():
            to_pair.wait_recv()
            crossed.start()
            crossed.wait_recv()

        pltpu.make_async_copy(h_ref.at[0, 0], hb.at[s, 2, t], rr_sem.at[2, k]).wait()
        for d in range(NX):
            column = msm[s, d, 0, t]
            picked = jnp.concatenate([held_x[0, column], held_x[1, column]], axis=0)
            product = lax.dot_general(
                picked, hb[s, d, t], (((1,), (1,)), ((), ())), preferred_element_type=jnp.float32
            ).astype(jnp.bfloat16)
            cb[s, d, 0, t] = product[:slab]
            cb[s, d, 1, t] = product[slab:]
        return carry

    def reach(i):
        free = i - 2 * LAG + 1
        held = jnp.where(inner, jnp.minimum(free, 2 * (i - HOLD)), free)
        return jnp.clip(held, 0, total)

    def step(i, carry):
        @pl.when(i < total)
        def _():
            s = i // cap
            t = lax.rem(i, cap)
            pltpu.make_async_copy(h_ref.at[0, 0], hb.at[s, 0, t], yr_sem.at[s, t]).wait()
            mine = hb.at[s, 0, t]
            remote(mine, hb.at[s, 3, t], rs_sem.at[0, s], rr_sem.at[3, i], x_up).start()
            remote(mine, hb.at[s, 1, t], rs_sem.at[1, s], rr_sem.at[1, i], x_down).start()

        @pl.when(jnp.logical_and(i >= LAG, i < total + LAG))
        def _():
            j = i - LAG
            s = j // cap
            t = lax.rem(j, cap)
            for d in (1, 3):
                pltpu.make_async_copy(h_ref.at[0, 0], hb.at[s, d, t], rr_sem.at[d, j]).wait()

            @pl.when(lax.rem(j, 2) == 0)
            def _():
                remote(hb.at[s, 3, t], hb.at[s, 2, t], fs_sem.at[0, s], rr_sem.at[2, j], x_up).start()

            @pl.when(lax.rem(j, 2) == 1)
            def _():
                remote(hb.at[s, 1, t], hb.at[s, 2, t], fs_sem.at[1, s], rr_sem.at[2, j], x_down).start()

        done, until = reach(i - 1), reach(i)
        lax.fori_loop(jnp.minimum(done, cap), jnp.minimum(until, cap), functools.partial(multiply, 0), 0)
        lax.fori_loop(jnp.maximum(done - cap, 0), jnp.maximum(until - cap, 0), functools.partial(multiply, 1), 0)
        return carry

    lax.fori_loop(0, total + 2 * LAG, step, 0)

    to_sibling.wait_send()
    to_pair.wait_send()
    forward_x.wait_send()
    pltpu.make_async_copy(h_ref.at[0], hb.at[0, 0], ys_sem.at[0]).wait()

    @pl.when(inner)
    def _():
        pltpu.make_async_copy(h_ref.at[0], hb.at[0, 0], ys_sem.at[1]).wait()

    send_chunk(jnp.int32(total // CHUNK - 1))
    for way in range(2):
        for s in range(2):
            pltpu.make_async_copy(h_ref.at[0], hb.at[s, 0], rs_sem.at[way, s]).wait()
            pltpu.make_async_copy(h_ref.at[0, pl.ds(0, cap // 2)], hb.at[s, 0, pl.ds(0, cap // 2)],
                                  fs_sem.at[way, s]).wait()
    for half in range(2):
        for d in range(NX):
            if d == 0:
                @pl.when(half * 2 + yh != y)
                def _(half=half, d=d):
                    pltpu.make_async_copy(m_ref, mbuf.at[0, 0], ms_sem.at[half, d]).wait()
            else:
                pltpu.make_async_copy(m_ref, mbuf.at[0, 0], ms_sem.at[half, d]).wait()
    for s in range(2):
        for dz in range(NX):
            for dc in range(2):
                if dz or dc:
                    pltpu.make_async_copy(mbuf.at[0, 0], mout_ref.at[0, 0, 0], ns_sem.at[s, dz, dc]).wait()
                    pltpu.make_async_copy(cb.at[0, 0, 0], out_ref.at[0, 0, 0], cs_sem.at[s, dz, dc]).wait()
    for c in range(2):
        for g in range(2):
            for q in range(NX):
                pltpu.make_async_copy(mbuf.at[0, 0], mout_ref.at[c, g, q], nr_sem.at[c, g, q]).wait()
                pltpu.make_async_copy(cb.at[0, 0, 0], out_ref.at[c, g, q], cr_sem.at[c, g, q]).wait()


def combine(cap, bs, slabs, steps, meta, coeffs, potential, c_ref, prev_ref, dens_ref, next_ref, dout_ref, even, odd):
    panel = pl.program_id(0)
    part = pl.program_id(1)
    columns = prev_ref.shape[0]
    width = prev_ref.shape[1]
    spare = even.shape[1] // bs - 1

    @pl.when(part == 0)
    def _():
        even[...] = jnp.zeros_like(even)
        odd[...] = jnp.zeros_like(odd)
        for q in range(NX):
            def add(t, carry):
                for g, acc in ((0, even), (1, odd)):
                    live = t < meta[panel, g, q, 2, 0]
                    row = pl.multiple_of(jnp.where(live, meta[panel, g, q, 1, t], spare) * bs, bs)
                    acc[:, pl.ds(row, bs)] += c_ref[0, g, q, t].astype(jnp.float32)
                return carry
            lax.fori_loop(0, jnp.maximum(meta[panel, 0, q, 2, 0], meta[panel, 1, q, 2, 0]), add, 0)

    height = columns // slabs
    base = pl.multiple_of(part * width, width)
    for s in range(slabs):
        rows = pl.ds(s * height, height)
        lanes = pl.ds(base, width)
        value = 2.0 * (even[rows, lanes] + odd[rows, lanes]) - prev_ref[rows, :]
        next_ref[rows, :] = value
        dout_ref[rows, :] = dens_ref[rows, :] + coeffs[potential[s]] * value


def shards(x_now, x_prev, density, coeffs, potential, h_tiles, tile_rows, tile_cols, tile_counts):
    columns, local_rows = x_now.shape
    cap = h_tiles.shape[1]
    bs = h_tiles.shape[-1]
    slabs = potential.shape[0]
    panel_rows = local_rows // bs // 2
    dma = pltpu.SemaphoreType.DMA
    bf16 = jnp.bfloat16
    anywhere = pl.BlockSpec(memory_space=pl.ANY)
    flops = 2 * 8 * cap * 2 * columns * bs * bs
    sums, places = pl.pallas_call(
        functools.partial(exchange, cap, columns, bs),
        out_shape=(
            jax.ShapeDtypeStruct((2, 2, NX, cap, columns, bs), bf16),
            jax.ShapeDtypeStruct((2, 2, NX, 8, 128), jnp.int32),
        ),
        in_specs=[anywhere, anywhere] + [pl.BlockSpec(memory_space=pltpu.VMEM)] * 3,
        out_specs=(anywhere, anywhere),
        scratch_shapes=[
            pltpu.VMEM((2, local_rows // bs, columns, bs), bf16),
            pltpu.VMEM((2, local_rows // bs, columns, bs), bf16),
            pltpu.VMEM((2, NX, cap, bs, bs), bf16),
            pltpu.VMEM((2, NX, 2, cap, columns, bs), bf16),
            pltpu.VMEM((8, 128), jnp.int32),
            pltpu.VMEM((2, NX, 8, 128), jnp.int32),
            pltpu.SMEM((2, NX, 8, 128), jnp.int32),
            dma((3,)), dma((3,)), dma,
            dma((2,)), dma((2, cap)),
            dma((2, 2)), dma((4, 2 * cap)), dma((2, 2)),
            dma((2, NX, 2)), dma((2, 2, NX)),
            dma((2, NX)), dma((2, NX)),
            dma((2, NX, 2)), dma((2, 2, NX)), dma,
        ],
        compiler_params=pltpu.CompilerParams(
            collective_id=0, has_side_effects=True, vmem_limit_bytes=56 * 1024 * 1024
        ),
        cost_estimate=pl.CostEstimate(flops=flops, bytes_accessed=16 * 1024 * 1024, transcendentals=0),
        name="exchange",
    )(x_now, h_tiles, tile_cols, tile_rows, tile_counts)
    parts = 4
    width = local_rows // 2 // parts
    wide = pl.BlockSpec((columns, width), lambda p, i, *_: (0, p * parts + i))
    return tuple(pl.pallas_call(
        functools.partial(combine, cap, bs, slabs, parts),
        out_shape=(
            jax.ShapeDtypeStruct((columns, local_rows), jnp.float32),
            jax.ShapeDtypeStruct((columns, local_rows), jnp.float32),
        ),
        grid_spec=pltpu.PrefetchScalarGridSpec(
            num_scalar_prefetch=3,
            grid=(2, parts),
            in_specs=[
                pl.BlockSpec((1, 2, NX, cap, columns, bs), lambda p, i, *_: (p, 0, 0, 0, 0, 0)),
                wide, wide,
            ],
            out_specs=(wide, wide),
            scratch_shapes=[pltpu.VMEM((columns, (panel_rows + 1) * bs), jnp.float32)] * 2,
        ),
        compiler_params=pltpu.CompilerParams(vmem_limit_bytes=48 * 1024 * 1024),
        cost_estimate=pl.CostEstimate(flops=8 * columns * local_rows, bytes_accessed=24 * 1024 * 1024,
                                      transcendentals=0),
        name="combine",
    )(places, coeffs, potential, sums, x_prev, density))


def solution(mesh):
    in_specs = (
        P("blk", "red"),
        P("blk", "red"),
        P("blk", "red"),
        P(),
        P("blk"),
        P("blk", "red", None, None),
        P("blk", "red"),
        P("blk", "red"),
        P("blk", "red"),
    )
    out_specs = (P("blk", "red"), P("blk", "red"))
    return jax.shard_map(shards, mesh=mesh, in_specs=in_specs, out_specs=out_specs, check_vma=False)
```

```python
import functools

import jax
import jax.numpy as jnp
from jax import lax
from jax.experimental import pallas as pl
from jax.experimental.pallas import tpu as pltpu
from jax.sharding import PartitionSpec as P

MESH = pl.DeviceIdType.MESH
NX = 4
LAG = 3
LAG2 = 2
HOLD = 9
RATE = 3
XL = 30
FAR = 7


def place():
    blk = lax.axis_index("blk")
    red = lax.axis_index("red")
    core = lax.rem(blk, 2)
    x = lax.rem(blk // 2, NX)
    yh = blk // (2 * NX)
    yl = red // NX
    z = lax.rem(red, NX)
    return x, yh, yl, z, core


def device(x, y, z, core):
    return ((y // 2) * (2 * NX) + x * 2 + core, lax.rem(y, 2) * NX + z)


def wrap(value):
    return lax.rem(value + 2 * NX, NX)


def exchange(cap, slab, bs, x_ref, h_ref, cols_ref, rows_ref, count_ref, out_ref, mout_ref, first_x, second_x, hb, cb, m_own, mbuf, msm,
             xs_sem, xr_sem, xl_sem, ys_sem, yr_sem, rs_sem, rr_sem, fs_sem, cs_sem, cr_sem,
             ms_sem, mr_sem, ns_sem, nr_sem, sm_sem):
    x, yh, yl, z, core = place()
    y = yh * 2 + yl
    other = 1 - core
    total = 2 * cap
    outer = jnp.logical_or(y == 0, y == 3)
    inner = jnp.logical_not(outer)

    def remote(src, dst, send, recv, to):
        return pltpu.make_async_remote_copy(
            src_ref=src, dst_ref=dst, send_sem=send, recv_sem=recv, device_id=to, device_id_type=MESH
        )

    here = (lax.axis_index("blk"), lax.axis_index("red"))
    sibling = device(x, y, z, other)
    x_up = device(wrap(x + 1), y, z, core)
    x_down = device(wrap(x - 1), y, z, core)
    y_pair = yh * 2 + (1 - yl)
    pair = device(x, y_pair, z, core)

    barrier = pltpu.get_barrier_semaphore()
    greeted = 0
    for dx in range(NX):
        for dy in range(NX):
            if dx or dy:
                pl.semaphore_signal(barrier, inc=1, device_id=device(wrap(x + dx), wrap(y + dy), z, core),
                                    device_id_type=MESH)
                greeted += 1
    for dz in range(NX):
        for dc in range(2):
            if dz or dc:
                to = device(x, y, wrap(z + dz), other if dc else core)
                pl.semaphore_signal(barrier, inc=1, device_id=to, device_id_type=MESH)
                greeted += 1
    blocks = first_x.shape[1]
    m_ref = m_own
    m_ref[...] = jnp.zeros(m_ref.shape, m_ref.dtype)
    m_ref[0:1, 0:cap] = cols_ref[...]
    m_ref[1:2, 0:cap] = rows_ref[...]
    m_ref[2:3, 0:1] = count_ref[...]

    def load_x(held):
        def one(b, carry):
            columns = pl.ds(pl.multiple_of(b * bs, bs), bs)
            pltpu.make_async_copy(x_ref.at[:, columns], held.at[core, b], xl_sem).start()
            return carry
        lax.fori_loop(0, blocks, one, 0)

    @pl.when(outer)
    def _():
        load_x(first_x)

    @pl.when(inner)
    def _():
        load_x(second_x)

    own_x = pltpu.make_async_copy(second_x.at[core], first_x.at[core], xl_sem)

    @pl.when(outer)
    def _():
        def load(t, carry):
            pltpu.make_async_copy(h_ref.at[0, t], hb.at[0, 0, t], yr_sem.at[0, t]).start()
            return carry
        lax.fori_loop(0, cap, load, 0)

    pl.semaphore_wait(barrier, greeted)

    for d in range(NX):
        for half in range(2):
            y_to = half * 2 + yh
            to_outer = jnp.logical_or(y_to == 0, y_to == 3)
            phase = jnp.where(to_outer == outer, 0, 1)
            to = device(wrap(x - d), y_to, z, core)
            if d == 0:
                @pl.when(y_to != y)
                def _(to=to, d=d, half=half, phase=phase):
                    remote(m_ref, mbuf.at[phase, d], ms_sem.at[half, d], mr_sem.at[phase, d], to).start()

                @pl.when(y_to == y)
                def _(d=d, phase=phase):
                    pltpu.make_async_copy(m_ref, mbuf.at[phase, d], mr_sem.at[phase, d]).start()
            else:
                remote(m_ref, mbuf.at[phase, d], ms_sem.at[half, d], mr_sem.at[phase, d], to).start()

    own_x.wait()
    far = device(x, wrap(y + 2), z, core)
    near = (pair, device(x, wrap(y_pair + 2), z, core))

    def x_copies(own, other_x):
        return (
            remote(own.at[core], own.at[core], xs_sem.at[0], xr_sem.at[0], sibling),
            remote(own.at[core], own.at[core], xs_sem.at[1], xr_sem.at[1], pair),
            remote(other_x.at[core], other_x.at[core], xs_sem.at[2], xr_sem.at[2], sibling),
        )

    to_sibling, to_pair, forward_x = x_copies(first_x, second_x)
    to_sibling_in, to_pair_in, forward_x_in = x_copies(second_x, first_x)

    @pl.when(outer)
    def _():
        to_pair.start()
        to_sibling.start()

    @pl.when(inner)
    def _():
        to_pair_in.start()
        to_sibling_in.start()

        def send(t, carry):
            remote(h_ref.at[0, t], hb.at[0, 0, t], ys_sem.at[1], yr_sem.at[0, t], near[1]).start()
            return carry
        lax.fori_loop(0, cap, send, 0)

        def send_near(t, carry):
            remote(h_ref.at[0, t], hb.at[1, 0, t], ys_sem.at[0], yr_sem.at[1, t], near[0]).start()
            return carry
        lax.fori_loop(0, cap, send_near, 0)

    for s in range(2):
        for d in range(NX):
            pltpu.make_async_copy(m_ref, mbuf.at[s, d], mr_sem.at[s, d]).wait()
    into_smem = pltpu.make_async_copy(mbuf, msm, sm_sem)
    into_smem.start()
    to_sibling.wait_recv()
    into_smem.wait()

    def side(s):
        return jnp.where((s == 0) == outer, yl, 1 - yl)

    for s in range(2):
        for dz in range(NX):
            z_to = wrap(z + dz)
            d = wrap(z_to - x)
            for dc in range(2):
                if dz or dc:
                    to = device(x, y, z_to, other if dc else core)
                    remote(mbuf.at[s, d], mout_ref.at[core, side(s), z], ns_sem.at[s, dz, dc],
                           nr_sem.at[core, side(s), z], to).start()
                else:
                    pltpu.make_async_copy(mbuf.at[s, d], mout_ref.at[core, side(s), z],
                                          nr_sem.at[core, side(s), z]).start()

    def multiply(s, owners, t, carry):
        held_x = second_x if s else first_x
        if owners == (0,):
            crossed = forward_x if s else forward_x_in

            @pl.when(jnp.logical_and(t == 0, outer if s else inner))
            def _():
                to_pair.wait_recv()
                crossed.start()
                crossed.wait_recv()

        for d in owners:
            if d == 2:
                pltpu.make_async_copy(h_ref.at[0, 0], hb.at[s, d, t], rr_sem.at[d, s * cap + t]).wait()
            column = msm[s, d, 0, t]
            picked = jnp.concatenate([held_x[0, column], held_x[1, column]], axis=0)
            product = lax.dot_general(
                picked, hb[s, d, t], (((1,), (1,)), ((), ())), preferred_element_type=jnp.float32
            ).astype(jnp.bfloat16)
            cb[s, d, 0, t] = product[:slab]
            cb[s, d, 1, t] = product[slab:]
        return carry

    def deliver(s, owners, t, carry):
        for d in owners:
            z_to = wrap(x + d)
            dst = out_ref.at[core, side(s), z, t]
            arrived = cr_sem.at[core, side(s), z]
            remote(cb.at[s, d, other, t], dst, cs_sem.at[s, d, 1], arrived, device(x, y, z_to, other)).start()

            @pl.when(z_to != z)
            def _(d=d, dst=dst, arrived=arrived, z_to=z_to):
                remote(cb.at[s, d, core, t], dst, cs_sem.at[s, d, 0], arrived, device(x, y, z_to, core)).start()

            @pl.when(z_to == z)
            def _(d=d, dst=dst, arrived=arrived):
                pltpu.make_async_copy(cb.at[s, d, core, t], dst, arrived).start()
        return carry

    kinds = (((0,), 0), ((1, 3), LAG), ((2,), LAG + LAG2))

    def reach(i, lag):
        free = i - lag + 1
        held = jnp.where(inner, jnp.minimum(free, RATE * (i - HOLD)), free)
        return jnp.clip(held, 0, total)

    def step(i, carry):
        @pl.when(jnp.logical_and(outer, jnp.logical_and(i >= FAR, i < FAR + cap)))
        def _():
            t = i - FAR
            remote(h_ref.at[0, t], hb.at[1, 0, t], ys_sem.at[0], yr_sem.at[1, t], far).start()

        @pl.when(i < total)
        def _():
            s = i // cap
            t = lax.rem(i, cap)
            pltpu.make_async_copy(h_ref.at[0, 0], hb.at[s, 0, t], yr_sem.at[s, t]).wait()
            mine = hb.at[s, 0, t]
            remote(mine, hb.at[s, 3, t], rs_sem.at[0, s], rr_sem.at[3, i], x_up).start()
            remote(mine, hb.at[s, 1, t], rs_sem.at[1, s], rr_sem.at[1, i], x_down).start()

        @pl.when(jnp.logical_and(i >= LAG, i < total + LAG))
        def _():
            j = i - LAG
            s = j // cap
            t = lax.rem(j, cap)
            for d in (1, 3):
                pltpu.make_async_copy(h_ref.at[0, 0], hb.at[s, d, t], rr_sem.at[d, j]).wait()

            @pl.when(lax.rem(j, 2) == 0)
            def _():
                remote(hb.at[s, 3, t], hb.at[s, 2, t], fs_sem.at[0, s], rr_sem.at[2, j], x_up).start()

            @pl.when(lax.rem(j, 2) == 1)
            def _():
                remote(hb.at[s, 1, t], hb.at[s, 2, t], fs_sem.at[1, s], rr_sem.at[2, j], x_down).start()

        for s in range(2):
            for work in (multiply, deliver):
                for owners, lag in kinds:
                    done = jnp.clip(reach(i - 1, lag) - s * cap, 0, cap)
                    until = jnp.clip(reach(i, lag) - s * cap, 0, cap)
                    lax.fori_loop(done, until, functools.partial(work, s, owners), 0)
        return carry

    lax.fori_loop(0, total + LAG + LAG2, step, 0)

    to_sibling.wait_send()
    to_pair.wait_send()
    forward_x.wait_send()
    pltpu.make_async_copy(h_ref.at[0], hb.at[0, 0], ys_sem.at[0]).wait()

    @pl.when(inner)
    def _():
        pltpu.make_async_copy(h_ref.at[0], hb.at[0, 0], ys_sem.at[1]).wait()

    for way in range(2):
        for s in range(2):
            pltpu.make_async_copy(h_ref.at[0], hb.at[s, 0], rs_sem.at[way, s]).wait()
            pltpu.make_async_copy(h_ref.at[0, pl.ds(0, cap // 2)], hb.at[s, 0, pl.ds(0, cap // 2)],
                                  fs_sem.at[way, s]).wait()
    for half in range(2):
        for d in range(NX):
            if d == 0:
                @pl.when(half * 2 + yh != y)
                def _(half=half, d=d):
                    pltpu.make_async_copy(m_ref, mbuf.at[0, 0], ms_sem.at[half, d]).wait()
            else:
                pltpu.make_async_copy(m_ref, mbuf.at[0, 0], ms_sem.at[half, d]).wait()
    for s in range(2):
        for dz in range(NX):
            for dc in range(2):
                if dz or dc:
                    pltpu.make_async_copy(mbuf.at[0, 0], mout_ref.at[0, 0, 0], ns_sem.at[s, dz, dc]).wait()
        for d in range(NX):
            pltpu.make_async_copy(cb.at[0, 0, 0], out_ref.at[0, 0, 0], cs_sem.at[s, d, 1]).wait()

            @pl.when(wrap(x + d) != z)
            def _(s=s, d=d):
                pltpu.make_async_copy(cb.at[0, 0, 0], out_ref.at[0, 0, 0], cs_sem.at[s, d, 0]).wait()
    for c in range(2):
        for g in range(2):
            for q in range(NX):
                pltpu.make_async_copy(mbuf.at[0, 0], mout_ref.at[c, g, q], nr_sem.at[c, g, q]).wait()
                pltpu.make_async_copy(cb.at[0, 0, 0], out_ref.at[c, g, q], cr_sem.at[c, g, q]).wait()


def combine(cap, bs, slabs, steps, meta, coeffs, potential, c_ref, prev_ref, dens_ref, next_ref, dout_ref, even, odd):
    panel = pl.program_id(0)
    part = pl.program_id(1)
    columns = prev_ref.shape[0]
    width = prev_ref.shape[1]
    spare = even.shape[1] // bs - 1

    @pl.when(part == 0)
    def _():
        even[...] = jnp.zeros_like(even)
        odd[...] = jnp.zeros_like(odd)
        for q in range(NX):
            def add(t, carry):
                for g, acc in ((0, even), (1, odd)):
                    live = t < meta[panel, g, q, 2, 0]
                    row = pl.multiple_of(jnp.where(live, meta[panel, g, q, 1, t], spare) * bs, bs)
                    acc[:, pl.ds(row, bs)] += c_ref[0, g, q, t].astype(jnp.float32)
                return carry
            lax.fori_loop(0, jnp.maximum(meta[panel, 0, q, 2, 0], meta[panel, 1, q, 2, 0]), add, 0)

    height = columns // slabs
    base = pl.multiple_of(part * width, width)
    for s in range(slabs):
        rows = pl.ds(s * height, height)
        lanes = pl.ds(base, width)
        value = 2.0 * (even[rows, lanes] + odd[rows, lanes]) - prev_ref[rows, :]
        next_ref[rows, :] = value
        dout_ref[rows, :] = dens_ref[rows, :] + coeffs[potential[s]] * value


def shards(x_now, x_prev, density, coeffs, potential, h_tiles, tile_rows, tile_cols, tile_counts):
    columns, local_rows = x_now.shape
    cap = h_tiles.shape[1]
    bs = h_tiles.shape[-1]
    slabs = potential.shape[0]
    panel_rows = local_rows // bs // 2
    dma = pltpu.SemaphoreType.DMA
    bf16 = jnp.bfloat16
    anywhere = pl.BlockSpec(memory_space=pl.ANY)
    flops = 2 * 8 * cap * 2 * columns * bs * bs
    sums, places = pl.pallas_call(
        functools.partial(exchange, cap, columns, bs),
        out_shape=(
            jax.ShapeDtypeStruct((2, 2, NX, cap, columns, bs), bf16),
            jax.ShapeDtypeStruct((2, 2, NX, 8, 128), jnp.int32),
        ),
        in_specs=[pl.BlockSpec(memory_space=pltpu.HBM)] * 2 + [pl.BlockSpec(memory_space=pltpu.VMEM)] * 3,
        out_specs=(anywhere, anywhere),
        scratch_shapes=[
            pltpu.VMEM((2, local_rows // bs, columns, bs), bf16),
            pltpu.VMEM((2, local_rows // bs, columns, bs), bf16),
            pltpu.VMEM((2, NX, cap, bs, bs), bf16),
            pltpu.VMEM((2, NX, 2, cap, columns, bs), bf16),
            pltpu.VMEM((8, 128), jnp.int32),
            pltpu.VMEM((2, NX, 8, 128), jnp.int32),
            pltpu.SMEM((2, NX, 8, 128), jnp.int32),
            dma((3,)), dma((3,)), dma,
            dma((2,)), dma((2, cap)),
            dma((2, 2)), dma((4, 2 * cap)), dma((2, 2)),
            dma((2, NX, 2)), dma((2, 2, NX)),
            dma((2, NX)), dma((2, NX)),
            dma((2, NX, 2)), dma((2, 2, NX)), dma,
        ],
        compiler_params=pltpu.CompilerParams(
            collective_id=0, has_side_effects=True, vmem_limit_bytes=XL * 1024 * 1024
        ),
        cost_estimate=pl.CostEstimate(flops=40 * flops, bytes_accessed=16 * 1024 * 1024, transcendentals=0),
        name="exchange",
    )(pltpu.with_memory_space_constraint(x_now, pltpu.HBM), pltpu.with_memory_space_constraint(h_tiles, pltpu.HBM), tile_cols, tile_rows, tile_counts)
    parts = 2
    width = local_rows // 2 // parts
    wide = pl.BlockSpec((columns, width), lambda p, i, *_: (0, p * parts + i))
    return tuple(pl.pallas_call(
        functools.partial(combine, cap, bs, slabs, parts),
        out_shape=(
            jax.ShapeDtypeStruct((columns, local_rows), jnp.float32),
            jax.ShapeDtypeStruct((columns, local_rows), jnp.float32),
        ),
        grid_spec=pltpu.PrefetchScalarGridSpec(
            num_scalar_prefetch=3,
            grid=(2, parts),
            in_specs=[
                pl.BlockSpec((1, 2, NX, cap, columns, bs), lambda p, i, *_: (p, 0, 0, 0, 0, 0)),
                wide, wide,
            ],
            out_specs=(wide, wide),
            scratch_shapes=[pltpu.VMEM((columns, (panel_rows + 1) * bs), jnp.float32)] * 2,
        ),
        compiler_params=pltpu.CompilerParams(vmem_limit_bytes=30 * 1024 * 1024),
        cost_estimate=pl.CostEstimate(flops=8 * columns * local_rows, bytes_accessed=24 * 1024 * 1024,
                                      transcendentals=0),
        name="combine",
    )(places, coeffs, potential, sums, x_prev, density))


def solution(mesh):
    in_specs = (
        P("blk", "red"),
        P("blk", "red"),
        P("blk", "red"),
        P(),
        P("blk"),
        P("blk", "red", None, None),
        P("blk", "red"),
        P("blk", "red"),
        P("blk", "red"),
    )
    out_specs = (P("blk", "red"), P("blk", "red"))
    return jax.shard_map(shards, mesh=mesh, in_specs=in_specs, out_specs=out_specs, check_vma=False)
```

```python
import functools

import jax
import jax.numpy as jnp
from jax import lax
from jax.experimental import pallas as pl
from jax.experimental.pallas import tpu as pltpu
from jax.sharding import PartitionSpec as P

MESH = pl.DeviceIdType.MESH
NX = 4
LAG = 3
LAG2 = 2
HOLD = 11
HOLD_LOW = 7
RATE = 3
XL = 30
FAR = 9


def place():
    blk = lax.axis_index("blk")
    red = lax.axis_index("red")
    core = lax.rem(blk, 2)
    x = lax.rem(blk // 2, NX)
    yh = blk // (2 * NX)
    yl = red // NX
    z = lax.rem(red, NX)
    return x, yh, yl, z, core


def device(x, y, z, core):
    return ((y // 2) * (2 * NX) + x * 2 + core, lax.rem(y, 2) * NX + z)


def wrap(value):
    return lax.rem(value + 2 * NX, NX)


def exchange(cap, slab, bs, x_ref, h_ref, cols_ref, rows_ref, count_ref, out_ref, mout_ref, first_lo, first_hi, second_lo, second_hi, hb, cb, m_own, mbuf, msm,
             xs_sem, xr_sem, xl_sem, ys_sem, yr_sem, rs_sem, rr_sem, fs_sem, cs_sem, cr_sem,
             ms_sem, mr_sem, ns_sem, nr_sem, sm_sem):
    x, yh, yl, z, core = place()
    y = yh * 2 + yl
    other = 1 - core
    total = 2 * cap
    outer = jnp.logical_or(y == 0, y == 3)
    inner = jnp.logical_not(outer)

    def remote(src, dst, send, recv, to):
        return pltpu.make_async_remote_copy(
            src_ref=src, dst_ref=dst, send_sem=send, recv_sem=recv, device_id=to, device_id_type=MESH
        )

    here = (lax.axis_index("blk"), lax.axis_index("red"))
    sibling = device(x, y, z, other)
    x_up = device(wrap(x + 1), y, z, core)
    x_down = device(wrap(x - 1), y, z, core)
    y_pair = yh * 2 + (1 - yl)
    pair = device(x, y_pair, z, core)

    barrier = pltpu.get_barrier_semaphore()
    greeted = 0
    for dx in range(NX):
        for dy in range(NX):
            if dx or dy:
                pl.semaphore_signal(barrier, inc=1, device_id=device(wrap(x + dx), wrap(y + dy), z, core),
                                    device_id_type=MESH)
                greeted += 1
    for dz in range(NX):
        for dc in range(2):
            if dz or dc:
                to = device(x, y, wrap(z + dz), other if dc else core)
                pl.semaphore_signal(barrier, inc=1, device_id=to, device_id_type=MESH)
                greeted += 1
    blocks = first_lo.shape[1]
    part = slab // 2
    first, second = (first_lo, first_hi), (second_lo, second_hi)
    m_ref = m_own
    m_ref[...] = jnp.zeros(m_ref.shape, m_ref.dtype)
    m_ref[0:1, 0:cap] = cols_ref[...]
    m_ref[1:2, 0:cap] = rows_ref[...]
    m_ref[2:3, 0:1] = count_ref[...]

    def load_x(held):
        def one(b, carry):
            columns = pl.ds(pl.multiple_of(b * bs, bs), bs)
            for h in range(2):
                rows = pl.ds(h * part, part)
                pltpu.make_async_copy(x_ref.at[rows, columns], held[h].at[core, b], xl_sem.at[h]).start()
            return carry
        lax.fori_loop(0, blocks, one, 0)

    @pl.when(outer)
    def _():
        load_x(first)

    @pl.when(inner)
    def _():
        load_x(second)

    own_x = [pltpu.make_async_copy(second[h].at[core], first[h].at[core], xl_sem.at[h]) for h in range(2)]

    @pl.when(outer)
    def _():
        def load(t, carry):
            pltpu.make_async_copy(h_ref.at[0, t], hb.at[0, 0, t], yr_sem.at[0, t]).start()
            return carry
        lax.fori_loop(0, cap, load, 0)

    pl.semaphore_wait(barrier, greeted)

    for d in range(NX):
        for half in range(2):
            y_to = half * 2 + yh
            to_outer = jnp.logical_or(y_to == 0, y_to == 3)
            phase = jnp.where(to_outer == outer, 0, 1)
            to = device(wrap(x - d), y_to, z, core)
            if d == 0:
                @pl.when(y_to != y)
                def _(to=to, d=d, half=half, phase=phase):
                    remote(m_ref, mbuf.at[phase, d], ms_sem.at[half, d], mr_sem.at[phase, d], to).start()

                @pl.when(y_to == y)
                def _(d=d, phase=phase):
                    pltpu.make_async_copy(m_ref, mbuf.at[phase, d], mr_sem.at[phase, d]).start()
            else:
                remote(m_ref, mbuf.at[phase, d], ms_sem.at[half, d], mr_sem.at[phase, d], to).start()

    for h in range(2):
        own_x[h].wait()
    pair_far = device(x, wrap(y_pair + 2), z, core)
    far = device(x, wrap(y + 2), z, core)
    near = (pair, pair_far)

    def x_copies(own, crossed):
        return (
            [remote(own[h].at[core], own[h].at[core], xs_sem.at[0, h], xr_sem.at[0, h], sibling) for h in range(2)],
            [remote(own[h].at[core], own[h].at[core], xs_sem.at[1, h], xr_sem.at[1, h], pair) for h in range(2)],
            [remote(crossed[h].at[core], crossed[h].at[core], xs_sem.at[2, h], xr_sem.at[2, h], sibling)
             for h in range(2)],
        )

    to_sibling, to_pair, forward_x = x_copies(first, second)
    to_sibling_in, to_pair_in, forward_x_in = x_copies(second, first)

    @pl.when(outer)
    def _():
        for h in range(2):
            to_pair[h].start()
        for h in range(2):
            to_sibling[h].start()

    @pl.when(inner)
    def _():
        for h in range(2):
            to_pair_in[h].start()
        for h in range(2):
            to_sibling_in[h].start()

        def send(t, carry):
            remote(h_ref.at[0, t], hb.at[0, 0, t], ys_sem.at[1], yr_sem.at[0, t], near[1]).start()
            return carry
        lax.fori_loop(0, cap, send, 0)

        def send_near(t, carry):
            remote(h_ref.at[0, t], hb.at[1, 0, t], ys_sem.at[0], yr_sem.at[1, t], near[0]).start()
            return carry
        lax.fori_loop(0, cap, send_near, 0)

    for s in range(2):
        for d in range(NX):
            pltpu.make_async_copy(m_ref, mbuf.at[s, d], mr_sem.at[s, d]).wait()
    into_smem = pltpu.make_async_copy(mbuf, msm, sm_sem)
    into_smem.start()
    for h in range(2):
        to_sibling[h].wait_recv()
    into_smem.wait()

    def side(s):
        return jnp.where((s == 0) == outer, yl, 1 - yl)

    for s in range(2):
        for dz in range(NX):
            z_to = wrap(z + dz)
            d = wrap(z_to - x)
            for dc in range(2):
                if dz or dc:
                    to = device(x, y, z_to, other if dc else core)
                    remote(mbuf.at[s, d], mout_ref.at[core, side(s), z], ns_sem.at[s, dz, dc],
                           nr_sem.at[core, side(s), z], to).start()
                else:
                    pltpu.make_async_copy(mbuf.at[s, d], mout_ref.at[core, side(s), z],
                                          nr_sem.at[core, side(s), z]).start()

    whole, low, high = (0, 1), (0,), (1,)

    def multiply(s, owners, halves, t, carry):
        held = second if s else first
        if owners == (0,):
            crossed = forward_x if s else forward_x_in

            @pl.when(jnp.logical_and(t == 0, outer if s else inner))
            def _():
                for h in halves:
                    to_pair[h].wait_recv()
                    crossed[h].start()
                for h in halves:
                    crossed[h].wait_recv()

        for d in owners:
            if d == 2 and halves != high:
                pltpu.make_async_copy(h_ref.at[0, 0], hb.at[s, d, t], rr_sem.at[d, s * cap + t]).wait()
            column = msm[s, d, 0, t]
            picked = jnp.concatenate([held[h][c, column] for c in range(2) for h in halves], axis=0)
            product = lax.dot_general(
                picked, hb[s, d, t], (((1,), (1,)), ((), ())), preferred_element_type=jnp.float32
            ).astype(jnp.bfloat16)
            count = part * len(halves)
            rows = pl.ds(halves[0] * part, count)
            cb[s, d, 0, t, rows] = product[:count]
            cb[s, d, 1, t, rows] = product[count:]
        return carry

    def deliver(s, owners, halves, t, carry):
        rows = pl.ds(halves[0] * part, part * len(halves))
        for d in owners:
            z_to = wrap(x + d)
            dst = out_ref.at[core, side(s), z, t, rows]
            theirs, mine = cb.at[s, d, other, t, rows], cb.at[s, d, core, t, rows]
            arrived = cr_sem.at[core, side(s), z]
            remote(theirs, dst, cs_sem.at[s, d, 1], arrived, device(x, y, z_to, other)).start()

            @pl.when(z_to != z)
            def _(d=d, dst=dst, arrived=arrived, z_to=z_to, mine=mine):
                remote(mine, dst, cs_sem.at[s, d, 0], arrived, device(x, y, z_to, core)).start()

            @pl.when(z_to == z)
            def _(dst=dst, arrived=arrived, mine=mine):
                pltpu.make_async_copy(mine, dst, arrived).start()
        return carry

    kinds = (((0,), 0), ((1, 3), LAG), ((2,), LAG + LAG2))

    def reach(i, lag, hold):
        free = i - lag + 1
        if hold is not None:
            free = jnp.minimum(free, RATE * (i - hold))
        return free

    passes = ((0, whole, None, outer), (0, low, HOLD_LOW, inner), (0, high, HOLD, inner), (1, whole, None, None))

    def span(i, s, lag, hold, who):
        free = reach(i, lag, hold) if s == 0 else jnp.where(
            outer, reach(i, lag, None), jnp.minimum(reach(i, lag, None), RATE * (i - HOLD)))
        free = jnp.clip(free - s * cap, 0, cap)
        return free if who is None else jnp.where(who, free, 0)

    def step(i, carry):
        @pl.when(jnp.logical_and(outer, jnp.logical_and(i >= FAR, i < FAR + cap)))
        def _():
            t = i - FAR
            remote(h_ref.at[0, t], hb.at[1, 0, t], ys_sem.at[0], yr_sem.at[1, t], far).start()

        @pl.when(i < total)
        def _():
            s = i // cap
            t = lax.rem(i, cap)
            pltpu.make_async_copy(h_ref.at[0, 0], hb.at[s, 0, t], yr_sem.at[s, t]).wait()
            mine = hb.at[s, 0, t]
            remote(mine, hb.at[s, 3, t], rs_sem.at[0, s], rr_sem.at[3, i], x_up).start()
            remote(mine, hb.at[s, 1, t], rs_sem.at[1, s], rr_sem.at[1, i], x_down).start()

        @pl.when(jnp.logical_and(i >= LAG, i < total + LAG))
        def _():
            j = i - LAG
            s = j // cap
            t = lax.rem(j, cap)
            for d in (1, 3):
                pltpu.make_async_copy(h_ref.at[0, 0], hb.at[s, d, t], rr_sem.at[d, j]).wait()

            @pl.when(lax.rem(j, 2) == 0)
            def _():
                remote(hb.at[s, 3, t], hb.at[s, 2, t], fs_sem.at[0, s], rr_sem.at[2, j], x_up).start()

            @pl.when(lax.rem(j, 2) == 1)
            def _():
                remote(hb.at[s, 1, t], hb.at[s, 2, t], fs_sem.at[1, s], rr_sem.at[2, j], x_down).start()

        for s, halves, hold, who in passes:
            for work in (multiply, deliver):
                for owners, lag in kinds:
                    done, until = span(i - 1, s, lag, hold, who), span(i, s, lag, hold, who)
                    lax.fori_loop(done, until, functools.partial(work, s, owners, halves), 0)
        return carry

    lax.fori_loop(0, total + LAG + LAG2, step, 0)

    for h in range(2):
        to_sibling[h].wait_send()
        to_pair[h].wait_send()
        forward_x[h].wait_send()
    pltpu.make_async_copy(h_ref.at[0], hb.at[0, 0], ys_sem.at[0]).wait()

    @pl.when(inner)
    def _():
        pltpu.make_async_copy(h_ref.at[0], hb.at[0, 0], ys_sem.at[1]).wait()

    for way in range(2):
        for s in range(2):
            pltpu.make_async_copy(h_ref.at[0], hb.at[s, 0], rs_sem.at[way, s]).wait()
            pltpu.make_async_copy(h_ref.at[0, pl.ds(0, cap // 2)], hb.at[s, 0, pl.ds(0, cap // 2)],
                                  fs_sem.at[way, s]).wait()
    for half in range(2):
        for d in range(NX):
            if d == 0:
                @pl.when(half * 2 + yh != y)
                def _(half=half, d=d):
                    pltpu.make_async_copy(m_ref, mbuf.at[0, 0], ms_sem.at[half, d]).wait()
            else:
                pltpu.make_async_copy(m_ref, mbuf.at[0, 0], ms_sem.at[half, d]).wait()
    for s in range(2):
        for dz in range(NX):
            for dc in range(2):
                if dz or dc:
                    pltpu.make_async_copy(mbuf.at[0, 0], mout_ref.at[0, 0, 0], ns_sem.at[s, dz, dc]).wait()
        for d in range(NX):
            pltpu.make_async_copy(cb.at[0, 0, 0], out_ref.at[0, 0, 0], cs_sem.at[s, d, 1]).wait()

            @pl.when(wrap(x + d) != z)
            def _(s=s, d=d):
                pltpu.make_async_copy(cb.at[0, 0, 0], out_ref.at[0, 0, 0], cs_sem.at[s, d, 0]).wait()
    for c in range(2):
        for g in range(2):
            for q in range(NX):
                pltpu.make_async_copy(mbuf.at[0, 0], mout_ref.at[c, g, q], nr_sem.at[c, g, q]).wait()
                pltpu.make_async_copy(cb.at[0, 0, 0], out_ref.at[c, g, q], cr_sem.at[c, g, q]).wait()


def combine(cap, bs, slabs, steps, meta, coeffs, potential, c_ref, prev_ref, dens_ref, next_ref, dout_ref, even, odd):
    panel = pl.program_id(0)
    part = pl.program_id(1)
    columns = prev_ref.shape[0]
    width = prev_ref.shape[1]
    spare = even.shape[1] // bs - 1

    @pl.when(part == 0)
    def _():
        even[...] = jnp.zeros_like(even)
        odd[...] = jnp.zeros_like(odd)
        for q in range(NX):
            def add(t, carry):
                for g, acc in ((0, even), (1, odd)):
                    live = t < meta[panel, g, q, 2, 0]
                    row = pl.multiple_of(jnp.where(live, meta[panel, g, q, 1, t], spare) * bs, bs)
                    acc[:, pl.ds(row, bs)] += c_ref[0, g, q, t].astype(jnp.float32)
                return carry
            lax.fori_loop(0, jnp.maximum(meta[panel, 0, q, 2, 0], meta[panel, 1, q, 2, 0]), add, 0)

    height = columns // slabs
    base = pl.multiple_of(part * width, width)
    for s in range(slabs):
        rows = pl.ds(s * height, height)
        lanes = pl.ds(base, width)
        value = 2.0 * (even[rows, lanes] + odd[rows, lanes]) - prev_ref[rows, :]
        next_ref[rows, :] = value
        dout_ref[rows, :] = dens_ref[rows, :] + coeffs[potential[s]] * value


def shards(x_now, x_prev, density, coeffs, potential, h_tiles, tile_rows, tile_cols, tile_counts):
    columns, local_rows = x_now.shape
    cap = h_tiles.shape[1]
    bs = h_tiles.shape[-1]
    slabs = potential.shape[0]
    panel_rows = local_rows // bs // 2
    dma = pltpu.SemaphoreType.DMA
    bf16 = jnp.bfloat16
    anywhere = pl.BlockSpec(memory_space=pl.ANY)
    flops = 2 * 8 * cap * 2 * columns * bs * bs
    sums, places = pl.pallas_call(
        functools.partial(exchange, cap, columns, bs),
        out_shape=(
            jax.ShapeDtypeStruct((2, 2, NX, cap, columns, bs), bf16),
            jax.ShapeDtypeStruct((2, 2, NX, 8, 128), jnp.int32),
        ),
        in_specs=[pl.BlockSpec(memory_space=pltpu.HBM)] * 2 + [pl.BlockSpec(memory_space=pltpu.VMEM)] * 3,
        out_specs=(anywhere, anywhere),
        scratch_shapes=[
            pltpu.VMEM((2, local_rows // bs, columns // 2, bs), bf16),
            pltpu.VMEM((2, local_rows // bs, columns // 2, bs), bf16),
            pltpu.VMEM((2, local_rows // bs, columns // 2, bs), bf16),
            pltpu.VMEM((2, local_rows // bs, columns // 2, bs), bf16),
            pltpu.VMEM((2, NX, cap, bs, bs), bf16),
            pltpu.VMEM((2, NX, 2, cap, columns, bs), bf16),
            pltpu.VMEM((8, 128), jnp.int32),
            pltpu.VMEM((2, NX, 8, 128), jnp.int32),
            pltpu.SMEM((2, NX, 8, 128), jnp.int32),
            dma((3, 2)), dma((3, 2)), dma((2,)),
            dma((2,)), dma((2, cap)),
            dma((2, 2)), dma((4, 2 * cap)), dma((2, 2)),
            dma((2, NX, 2)), dma((2, 2, NX)),
            dma((2, NX)), dma((2, NX)),
            dma((2, NX, 2)), dma((2, 2, NX)), dma,
        ],
        compiler_params=pltpu.CompilerParams(
            collective_id=0, has_side_effects=True, vmem_limit_bytes=XL * 1024 * 1024
        ),
        cost_estimate=pl.CostEstimate(flops=40 * flops, bytes_accessed=16 * 1024 * 1024, transcendentals=0),
        name="exchange",
    )(pltpu.with_memory_space_constraint(x_now, pltpu.HBM), pltpu.with_memory_space_constraint(h_tiles, pltpu.HBM), tile_cols, tile_rows, tile_counts)
    parts = 1
    width = local_rows // 2 // parts
    wide = pl.BlockSpec((columns, width), lambda p, i, *_: (0, p * parts + i))
    return tuple(pl.pallas_call(
        functools.partial(combine, cap, bs, slabs, parts),
        out_shape=(
            jax.ShapeDtypeStruct((columns, local_rows), jnp.float32),
            jax.ShapeDtypeStruct((columns, local_rows), jnp.float32),
        ),
        grid_spec=pltpu.PrefetchScalarGridSpec(
            num_scalar_prefetch=3,
            grid=(2, parts),
            in_specs=[
                pl.BlockSpec((1, 2, NX, cap, columns, bs), lambda p, i, *_: (p, 0, 0, 0, 0, 0)),
                wide, wide,
            ],
            out_specs=(wide, wide),
            scratch_shapes=[pltpu.VMEM((columns, (panel_rows + 1) * bs), jnp.float32)] * 2,
        ),
        compiler_params=pltpu.CompilerParams(vmem_limit_bytes=30 * 1024 * 1024),
        cost_estimate=pl.CostEstimate(flops=8 * columns * local_rows, bytes_accessed=24 * 1024 * 1024,
                                      transcendentals=0),
        name="combine",
    )(places, coeffs, potential, sums, x_prev, density))


def solution(mesh):
    in_specs = (
        P("blk", "red"),
        P("blk", "red"),
        P("blk", "red"),
        P(),
        P("blk"),
        P("blk", "red", None, None),
        P("blk", "red"),
        P("blk", "red"),
        P("blk", "red"),
    )
    out_specs = (P("blk", "red"), P("blk", "red"))
    return jax.shard_map(shards, mesh=mesh, in_specs=in_specs, out_specs=out_specs, check_vma=False)
```

```python
import functools

import jax
import jax.numpy as jnp
from jax import lax
from jax.experimental import pallas as pl
from jax.experimental.pallas import tpu as pltpu
from jax.sharding import PartitionSpec as P

MESH = pl.DeviceIdType.MESH
NX = 4
LAG = 3
LAG2 = 3
HOLD = 12
HOLD_LOW = 8
RATE = 3
XL = 30
FAR = 9
EARLY = 2


def place():
    blk = lax.axis_index("blk")
    red = lax.axis_index("red")
    core = lax.rem(blk, 2)
    x = lax.rem(blk // 2, NX)
    yh = blk // (2 * NX)
    yl = red // NX
    z = lax.rem(red, NX)
    return x, yh, yl, z, core


def device(x, y, z, core):
    return ((y // 2) * (2 * NX) + x * 2 + core, lax.rem(y, 2) * NX + z)


def wrap(value):
    return lax.rem(value + 2 * NX, NX)


def exchange(cap, slab, bs, x_ref, h_ref, cols_ref, rows_ref, count_ref, out_ref, mout_ref, first_lo, first_hi, second_lo, second_hi, hb, cb, m_own, mbuf, msm,
             xs_sem, xr_sem, xl_sem, ys_sem, yr_sem, rs_sem, rr_sem, fs_sem, cs_sem, cr_sem,
             ms_sem, mr_sem, ns_sem, nr_sem, sm_sem):
    x, yh, yl, z, core = place()
    y = yh * 2 + yl
    other = 1 - core
    total = 2 * cap
    outer = jnp.logical_or(y == 0, y == 3)
    inner = jnp.logical_not(outer)

    def remote(src, dst, send, recv, to):
        return pltpu.make_async_remote_copy(
            src_ref=src, dst_ref=dst, send_sem=send, recv_sem=recv, device_id=to, device_id_type=MESH
        )

    here = (lax.axis_index("blk"), lax.axis_index("red"))
    sibling = device(x, y, z, other)
    x_up = device(wrap(x + 1), y, z, core)
    x_down = device(wrap(x - 1), y, z, core)
    y_pair = yh * 2 + (1 - yl)
    pair = device(x, y_pair, z, core)

    barrier = pltpu.get_barrier_semaphore()
    greeted = 0
    for dx in range(NX):
        for dy in range(NX):
            if dx or dy:
                pl.semaphore_signal(barrier, inc=1, device_id=device(wrap(x + dx), wrap(y + dy), z, core),
                                    device_id_type=MESH)
                greeted += 1
    for dz in range(NX):
        for dc in range(2):
            if dz or dc:
                to = device(x, y, wrap(z + dz), other if dc else core)
                pl.semaphore_signal(barrier, inc=1, device_id=to, device_id_type=MESH)
                greeted += 1
    blocks = first_lo.shape[1]
    part = slab // 2
    first, second = (first_lo, first_hi), (second_lo, second_hi)
    m_ref = m_own
    m_ref[...] = jnp.zeros(m_ref.shape, m_ref.dtype)
    m_ref[0:1, 0:cap] = cols_ref[...]
    m_ref[1:2, 0:cap] = rows_ref[...]
    m_ref[2:3, 0:1] = count_ref[...]

    def load_x(held):
        def one(b, carry):
            columns = pl.ds(pl.multiple_of(b * bs, bs), bs)
            for h in range(2):
                rows = pl.ds(h * part, part)
                pltpu.make_async_copy(x_ref.at[rows, columns], held[h].at[core, b], xl_sem.at[h]).start()
            return carry
        lax.fori_loop(0, blocks, one, 0)

    @pl.when(outer)
    def _():
        load_x(first)

    @pl.when(inner)
    def _():
        load_x(second)

    own_x = [pltpu.make_async_copy(second[h].at[core], first[h].at[core], xl_sem.at[h]) for h in range(2)]

    @pl.when(outer)
    def _():
        def load(t, carry):
            pltpu.make_async_copy(h_ref.at[0, t], hb.at[0, 0, t], yr_sem.at[0, t]).start()
            return carry
        lax.fori_loop(0, cap, load, 0)

    pl.semaphore_wait(barrier, greeted)
    far = device(x, wrap(y + 2), z, core)
    near = (pair, device(x, wrap(y_pair + 2), z, core))

    for d in range(NX):
        for half in range(2):
            y_to = half * 2 + yh
            to_outer = jnp.logical_or(y_to == 0, y_to == 3)
            phase = jnp.where(to_outer == outer, 0, 1)
            to = device(wrap(x - d), y_to, z, core)
            if d == 0:
                @pl.when(y_to != y)
                def _(to=to, d=d, half=half, phase=phase):
                    remote(m_ref, mbuf.at[phase, d], ms_sem.at[half, d], mr_sem.at[phase, d], to).start()

                @pl.when(y_to == y)
                def _(d=d, phase=phase):
                    pltpu.make_async_copy(m_ref, mbuf.at[phase, d], mr_sem.at[phase, d]).start()
            else:
                remote(m_ref, mbuf.at[phase, d], ms_sem.at[half, d], mr_sem.at[phase, d], to).start()

    @pl.when(inner)
    def _():
        def send(t, carry):
            remote(h_ref.at[0, t], hb.at[0, 0, t], ys_sem.at[1], yr_sem.at[0, t], near[1]).start()
            return carry
        lax.fori_loop(0, cap, send, 0)

    for h in range(2):
        own_x[h].wait()
    def x_copies(own, crossed):
        return (
            [remote(own[h].at[core], own[h].at[core], xs_sem.at[0, h], xr_sem.at[0, h], sibling) for h in range(2)],
            [remote(own[h].at[core], own[h].at[core], xs_sem.at[1, h], xr_sem.at[1, h], pair) for h in range(2)],
            [remote(crossed[h].at[core], crossed[h].at[core], xs_sem.at[2, h], xr_sem.at[2, h], sibling)
             for h in range(2)],
        )

    to_sibling, to_pair, forward_x = x_copies(first, second)
    to_sibling_in, to_pair_in, forward_x_in = x_copies(second, first)

    @pl.when(outer)
    def _():
        for h in range(2):
            to_pair[h].start()
        for h in range(2):
            to_sibling[h].start()

    @pl.when(inner)
    def _():
        for h in range(2):
            to_pair_in[h].start()
        for h in range(2):
            to_sibling_in[h].start()

        def send_near(t, carry):
            remote(h_ref.at[0, t], hb.at[1, 0, t], ys_sem.at[0], yr_sem.at[1, t], near[0]).start()
            return carry
        lax.fori_loop(0, cap, send_near, 0)

    def side(s):
        return jnp.where((s == 0) == outer, yl, 1 - yl)

    def positions():
        for s in range(2):
            for d in range(NX):
                pltpu.make_async_copy(m_ref, mbuf.at[s, d], mr_sem.at[s, d]).wait()
        into_smem = pltpu.make_async_copy(mbuf, msm, sm_sem)
        into_smem.start()
        for h in range(2):
            to_sibling[h].wait_recv()
        into_smem.wait()

        for s in range(2):
            for dz in range(NX):
                z_to = wrap(z + dz)
                d = wrap(z_to - x)
                for dc in range(2):
                    if dz or dc:
                        to = device(x, y, z_to, other if dc else core)
                        remote(mbuf.at[s, d], mout_ref.at[core, side(s), z], ns_sem.at[s, dz, dc],
                               nr_sem.at[core, side(s), z], to).start()
                    else:
                        pltpu.make_async_copy(mbuf.at[s, d], mout_ref.at[core, side(s), z],
                                              nr_sem.at[core, side(s), z]).start()

    whole, low, high = (0, 1), (0,), (1,)

    def multiply(s, owners, halves, t, carry):
        held = second if s else first
        if owners == (0,):
            crossed = forward_x if s else forward_x_in

            @pl.when(jnp.logical_and(t == 0, outer if s else inner))
            def _():
                for h in halves:
                    to_pair[h].wait_recv()
                    crossed[h].start()
                for h in halves:
                    crossed[h].wait_recv()

        for d in owners:
            if d == 2 and halves != high:
                pltpu.make_async_copy(h_ref.at[0, 0], hb.at[s, d, t], rr_sem.at[d, s * cap + t]).wait()
            column = msm[s, d, 0, t]
            picked = jnp.concatenate([held[h][c, column] for c in range(2) for h in halves], axis=0)
            product = lax.dot_general(
                picked, hb[s, d, t], (((1,), (1,)), ((), ())), preferred_element_type=jnp.float32
            ).astype(jnp.bfloat16)
            count = part * len(halves)
            rows = pl.ds(halves[0] * part, count)
            cb[s, d, 0, t, rows] = product[:count]
            cb[s, d, 1, t, rows] = product[count:]
        return carry

    def deliver(s, owners, halves, t, carry):
        rows = pl.ds(halves[0] * part, part * len(halves))
        for d in owners:
            z_to = wrap(x + d)
            dst = out_ref.at[core, side(s), z, t, rows]
            theirs, mine = cb.at[s, d, other, t, rows], cb.at[s, d, core, t, rows]
            arrived = cr_sem.at[core, side(s), z]
            remote(theirs, dst, cs_sem.at[s, d, 1], arrived, device(x, y, z_to, other)).start()

            @pl.when(z_to != z)
            def _(d=d, dst=dst, arrived=arrived, z_to=z_to, mine=mine):
                remote(mine, dst, cs_sem.at[s, d, 0], arrived, device(x, y, z_to, core)).start()

            @pl.when(z_to == z)
            def _(dst=dst, arrived=arrived, mine=mine):
                pltpu.make_async_copy(mine, dst, arrived).start()
        return carry

    kinds = (((0,), EARLY), ((1, 3), LAG), ((2,), LAG + LAG2))

    def reach(i, lag, hold):
        free = i - lag + 1
        if hold is not None:
            free = jnp.minimum(free, RATE * (i - hold))
        return free

    passes = ((0, whole, None, outer), (0, low, HOLD_LOW, inner), (0, high, HOLD, inner), (1, whole, None, None))

    def span(i, s, lag, hold, who):
        free = reach(i, lag, hold) if s == 0 else jnp.where(
            outer, reach(i, lag, None), jnp.minimum(reach(i, lag, None), RATE * (i - HOLD)))
        free = jnp.clip(free - s * cap, 0, cap)
        return free if who is None else jnp.where(who, free, 0)

    def step(i, carry):
        @pl.when(jnp.logical_and(outer, jnp.logical_and(i >= FAR, i < FAR + cap)))
        def _():
            t = i - FAR
            remote(h_ref.at[0, t], hb.at[1, 0, t], ys_sem.at[0], yr_sem.at[1, t], far).start()

        @pl.when(i < total)
        def _():
            s = i // cap
            t = lax.rem(i, cap)
            pltpu.make_async_copy(h_ref.at[0, 0], hb.at[s, 0, t], yr_sem.at[s, t]).wait()
            mine = hb.at[s, 0, t]
            remote(mine, hb.at[s, 3, t], rs_sem.at[0, s], rr_sem.at[3, i], x_up).start()
            remote(mine, hb.at[s, 1, t], rs_sem.at[1, s], rr_sem.at[1, i], x_down).start()

        @pl.when(jnp.logical_and(i >= LAG, i < total + LAG))
        def _():
            j = i - LAG
            s = j // cap
            t = lax.rem(j, cap)
            for d in (1, 3):
                pltpu.make_async_copy(h_ref.at[0, 0], hb.at[s, d, t], rr_sem.at[d, j]).wait()

            @pl.when(lax.rem(j, 2) == 0)
            def _():
                remote(hb.at[s, 3, t], hb.at[s, 2, t], fs_sem.at[0, s], rr_sem.at[2, j], x_up).start()

            @pl.when(lax.rem(j, 2) == 1)
            def _():
                remote(hb.at[s, 1, t], hb.at[s, 2, t], fs_sem.at[1, s], rr_sem.at[2, j], x_down).start()

        @pl.when(i == EARLY)
        def _():
            positions()

        for s, halves, hold, who in passes:
            for work in (multiply, deliver):
                for owners, lag in kinds:
                    done, until = span(i - 1, s, lag, hold, who), span(i, s, lag, hold, who)
                    lax.fori_loop(done, until, functools.partial(work, s, owners, halves), 0)
        return carry

    lax.fori_loop(0, total + LAG + LAG2, step, 0)

    for h in range(2):
        to_sibling[h].wait_send()
        to_pair[h].wait_send()
        forward_x[h].wait_send()
    pltpu.make_async_copy(h_ref.at[0], hb.at[0, 0], ys_sem.at[0]).wait()

    @pl.when(inner)
    def _():
        pltpu.make_async_copy(h_ref.at[0], hb.at[0, 0], ys_sem.at[1]).wait()

    for way in range(2):
        for s in range(2):
            pltpu.make_async_copy(h_ref.at[0], hb.at[s, 0], rs_sem.at[way, s]).wait()
            pltpu.make_async_copy(h_ref.at[0, pl.ds(0, cap // 2)], hb.at[s, 0, pl.ds(0, cap // 2)],
                                  fs_sem.at[way, s]).wait()
    for half in range(2):
        for d in range(NX):
            if d == 0:
                @pl.when(half * 2 + yh != y)
                def _(half=half, d=d):
                    pltpu.make_async_copy(m_ref, mbuf.at[0, 0], ms_sem.at[half, d]).wait()
            else:
                pltpu.make_async_copy(m_ref, mbuf.at[0, 0], ms_sem.at[half, d]).wait()
    for s in range(2):
        for dz in range(NX):
            for dc in range(2):
                if dz or dc:
                    pltpu.make_async_copy(mbuf.at[0, 0], mout_ref.at[0, 0, 0], ns_sem.at[s, dz, dc]).wait()
        for d in range(NX):
            pltpu.make_async_copy(cb.at[0, 0, 0], out_ref.at[0, 0, 0], cs_sem.at[s, d, 1]).wait()

            @pl.when(wrap(x + d) != z)
            def _(s=s, d=d):
                pltpu.make_async_copy(cb.at[0, 0, 0], out_ref.at[0, 0, 0], cs_sem.at[s, d, 0]).wait()
    for c in range(2):
        for g in range(2):
            for q in range(NX):
                pltpu.make_async_copy(mbuf.at[0, 0], mout_ref.at[c, g, q], nr_sem.at[c, g, q]).wait()
                pltpu.make_async_copy(cb.at[0, 0, 0], out_ref.at[c, g, q], cr_sem.at[c, g, q]).wait()


def combine(cap, bs, slabs, steps, meta, coeffs, potential, c_ref, prev_ref, dens_ref, next_ref, dout_ref, even, odd):
    panel = pl.program_id(0)
    part = pl.program_id(1)
    columns = prev_ref.shape[0]
    width = prev_ref.shape[1]
    spare = even.shape[1] // bs - 1

    @pl.when(part == 0)
    def _():
        even[...] = jnp.zeros_like(even)
        odd[...] = jnp.zeros_like(odd)
        for q in range(NX):
            def add(t, carry):
                for g, acc in ((0, even), (1, odd)):
                    live = t < meta[panel, g, q, 2, 0]
                    row = pl.multiple_of(jnp.where(live, meta[panel, g, q, 1, t], spare) * bs, bs)
                    acc[:, pl.ds(row, bs)] += c_ref[0, g, q, t].astype(jnp.float32)
                return carry
            lax.fori_loop(0, jnp.maximum(meta[panel, 0, q, 2, 0], meta[panel, 1, q, 2, 0]), add, 0)

    height = columns // slabs
    base = pl.multiple_of(part * width, width)
    for s in range(slabs):
        rows = pl.ds(s * height, height)
        lanes = pl.ds(base, width)
        value = 2.0 * (even[rows, lanes] + odd[rows, lanes]) - prev_ref[rows, :]
        next_ref[rows, :] = value
        dout_ref[rows, :] = dens_ref[rows, :] + coeffs[potential[s]] * value


def shards(x_now, x_prev, density, coeffs, potential, h_tiles, tile_rows, tile_cols, tile_counts):
    columns, local_rows = x_now.shape
    cap = h_tiles.shape[1]
    bs = h_tiles.shape[-1]
    slabs = potential.shape[0]
    panel_rows = local_rows // bs // 2
    dma = pltpu.SemaphoreType.DMA
    bf16 = jnp.bfloat16
    anywhere = pl.BlockSpec(memory_space=pl.ANY)
    flops = 2 * 8 * cap * 2 * columns * bs * bs
    sums, places = pl.pallas_call(
        functools.partial(exchange, cap, columns, bs),
        out_shape=(
            jax.ShapeDtypeStruct((2, 2, NX, cap, columns, bs), bf16),
            jax.ShapeDtypeStruct((2, 2, NX, 8, 128), jnp.int32),
        ),
        in_specs=[pl.BlockSpec(memory_space=pltpu.HBM)] * 2 + [pl.BlockSpec(memory_space=pltpu.VMEM)] * 3,
        out_specs=(anywhere, anywhere),
        scratch_shapes=[
            pltpu.VMEM((2, local_rows // bs, columns // 2, bs), bf16),
            pltpu.VMEM((2, local_rows // bs, columns // 2, bs), bf16),
            pltpu.VMEM((2, local_rows // bs, columns // 2, bs), bf16),
            pltpu.VMEM((2, local_rows // bs, columns // 2, bs), bf16),
            pltpu.VMEM((2, NX, cap, bs, bs), bf16),
            pltpu.VMEM((2, NX, 2, cap, columns, bs), bf16),
            pltpu.VMEM((8, 128), jnp.int32),
            pltpu.VMEM((2, NX, 8, 128), jnp.int32),
            pltpu.SMEM((2, NX, 8, 128), jnp.int32),
            dma((3, 2)), dma((3, 2)), dma((2,)),
            dma((2,)), dma((2, cap)),
            dma((2, 2)), dma((4, 2 * cap)), dma((2, 2)),
            dma((2, NX, 2)), dma((2, 2, NX)),
            dma((2, NX)), dma((2, NX)),
            dma((2, NX, 2)), dma((2, 2, NX)), dma,
        ],
        compiler_params=pltpu.CompilerParams(
            collective_id=0, has_side_effects=True, vmem_limit_bytes=XL * 1024 * 1024
        ),
        cost_estimate=pl.CostEstimate(flops=40 * flops, bytes_accessed=16 * 1024 * 1024, transcendentals=0),
        name="exchange",
    )(pltpu.with_memory_space_constraint(x_now, pltpu.HBM), pltpu.with_memory_space_constraint(h_tiles, pltpu.HBM),
      pltpu.with_memory_space_constraint(tile_cols, pltpu.HBM), pltpu.with_memory_space_constraint(tile_rows, pltpu.HBM), tile_counts)
    parts = 1
    width = local_rows // 2 // parts
    wide = pl.BlockSpec((columns, width), lambda p, i, *_: (0, p * parts + i))
    return tuple(pl.pallas_call(
        functools.partial(combine, cap, bs, slabs, parts),
        out_shape=(
            jax.ShapeDtypeStruct((columns, local_rows), jnp.float32),
            jax.ShapeDtypeStruct((columns, local_rows), jnp.float32),
        ),
        grid_spec=pltpu.PrefetchScalarGridSpec(
            num_scalar_prefetch=3,
            grid=(2, parts),
            in_specs=[
                pl.BlockSpec((1, 2, NX, cap, columns, bs), lambda p, i, *_: (p, 0, 0, 0, 0, 0)),
                wide, wide,
            ],
            out_specs=(wide, wide),
            scratch_shapes=[pltpu.VMEM((columns, (panel_rows + 1) * bs), jnp.float32)] * 2,
        ),
        compiler_params=pltpu.CompilerParams(vmem_limit_bytes=30 * 1024 * 1024),
        cost_estimate=pl.CostEstimate(flops=8 * columns * local_rows, bytes_accessed=24 * 1024 * 1024,
                                      transcendentals=0),
        name="combine",
    )(places, coeffs, potential, sums, x_prev, density))


def solution(mesh):
    in_specs = (
        P("blk", "red"),
        P("blk", "red"),
        P("blk", "red"),
        P(),
        P("blk"),
        P("blk", "red", None, None),
        P("blk", "red"),
        P("blk", "red"),
        P("blk", "red"),
    )
    out_specs = (P("blk", "red"), P("blk", "red"))
    return jax.shard_map(shards, mesh=mesh, in_specs=in_specs, out_specs=out_specs, check_vma=False)
```
